16 devices in a mesh: data: 2 (over y, z), seq: 8 (over x, core).
Axes of the slice: x: 4, y: 2, z: 1, core: 2. Of those that a mesh axis runs over, the one named last changes fastest.
The devices are a block of a 4x4x8 slice.
Arguments:
- x_in: bfloat16 [12, 2048, 2048], P(None, ('data', 'seq')), parts along dimension 1
- positions: int32 [2048], P(('data', 'seq')), parts along dimension 0
- w_query: bfloat16 [3, 2048, 24, 128], replicated
- w_key: bfloat16 [3, 2048, 24, 128], replicated
- w_value: bfloat16 [3, 2048, 24, 128], replicated
- w_out: bfloat16 [3, 24, 128, 2048], replicated
- w_up: bfloat16 [3, 2048, 8192], replicated
- w_down: bfloat16 [3, 8192, 2048], replicated
- g_attn: float32 [3, 2048], replicated
- g_mlp: float32 [3, 2048], replicated
Outputs:
- output: bfloat16 [12, 2048, 2048], P(None, ('data', 'seq')), parts along dimension 1
There are 2 independent parts. The reference program is written for one: setup_inputs(seed, part) draws one part's arguments, and reference() takes and returns one part's arrays. A program takes and returns all parts, laid end to end along the dimension named above; an argument that names none is the same for every part.
All inputs are finite; a program needn't handle non-finite values.
Results may differ from the reference program's by a relative error of at most 0.0147716.
Values are sent between devices in bfloat16 or wider.
A program may use at most 768 MiB of HBM per device.

```python
import jax
import jax.numpy as jnp
from jax import lax

BATCH_SIZE = 12
SEQ_LEN = 1024
D_MODEL = 2048
N_HEADS = 24
N_KV_HEADS = 24
HEAD_DIM = 128
FF_DIM = 8192
N_LAYERS = 3
REF_BLOCK = 64

ROPE_BASE = 10000.0
NORM_EPS = 1e-6


def normal_weights(rng_key, w_shape, fan_in, w_gain):
    return (jax.random.normal(rng_key, w_shape, jnp.float32) * (w_gain * fan_in ** -0.5)).astype(jnp.bfloat16)


def setup_inputs(seed: int = 0, part: int = 0) -> dict:
    base_key = jax.random.key(seed)
    part_keys = jax.random.split(jax.random.fold_in(base_key, part), 6)
    weight_keys = jax.random.split(jax.random.fold_in(base_key, 100003), 8)
    step_frac = jnp.arange(SEQ_LEN, dtype=jnp.float32) / SEQ_LEN
    wave_freq = jax.random.uniform(part_keys[0], (BATCH_SIZE, 4), jnp.float32, minval=0.5, maxval=3.0)
    wave_phase = jax.random.uniform(part_keys[1], (BATCH_SIZE, 4), jnp.float32, minval=0.0, maxval=6.283185)
    wave_vals = jnp.cos(6.283185 * wave_freq[:, :, None] * step_frac[None, None, :] + wave_phase[:, :, None])
    wave_dirs = jax.random.normal(part_keys[2], (BATCH_SIZE, 4, D_MODEL), jnp.float32)
    smooth = jnp.einsum("bjs,bjd->bsd", wave_vals, wave_dirs) * 0.5
    noise_part = jax.random.normal(part_keys[3], (BATCH_SIZE, SEQ_LEN, D_MODEL), jnp.float32) * 0.7
    offset = jax.random.randint(part_keys[4], (), 0, SEQ_LEN)
    pos_gaps = jax.random.randint(part_keys[5], (SEQ_LEN,), 1, 5)
    return {
        "x_in": (smooth + noise_part).astype(jnp.bfloat16),
        "positions": (offset + jnp.cumsum(pos_gaps)).astype(jnp.int32),
        "w_query": normal_weights(weight_keys[0], (N_LAYERS, D_MODEL, N_HEADS, HEAD_DIM), D_MODEL, 1.25),
        "w_key": normal_weights(weight_keys[1], (N_LAYERS, D_MODEL, N_KV_HEADS, HEAD_DIM), D_MODEL, 1.25),
        "w_value": normal_weights(weight_keys[2], (N_LAYERS, D_MODEL, N_KV_HEADS, HEAD_DIM), D_MODEL, 1.0),
        "w_out": normal_weights(weight_keys[3], (N_LAYERS, N_HEADS, HEAD_DIM, D_MODEL), N_HEADS * HEAD_DIM, 1.0),
        "w_up": normal_weights(weight_keys[4], (N_LAYERS, D_MODEL, FF_DIM), D_MODEL, 1.0),
        "w_down": normal_weights(weight_keys[5], (N_LAYERS, FF_DIM, D_MODEL), FF_DIM, 1.0),
        "g_attn": jax.random.uniform(weight_keys[6], (N_LAYERS, D_MODEL), jnp.float32, minval=0.5, maxval=1.5),
        "g_mlp": jax.random.uniform(weight_keys[7], (N_LAYERS, D_MODEL), jnp.float32, minval=0.5, maxval=1.5),
    }


def rms_norm(x_act, gain_vec):
    x_f32 = x_act.astype(jnp.float32)
    mean_sq = jnp.mean(x_f32 * x_f32, axis=-1, keepdims=True)
    return (x_f32 * lax.rsqrt(mean_sq + NORM_EPS) * gain_vec).astype(jnp.bfloat16)


def rope_tables(positions):
    inv_freq = ROPE_BASE ** (-jnp.arange(HEAD_DIM // 2, dtype=jnp.float32) * (2.0 / HEAD_DIM))
    angles = positions.astype(jnp.float32)[:, None] * inv_freq[None, :]
    return jnp.cos(angles), jnp.sin(angles)


def apply_rope(proj_f32, cos_t, sin_t):
    half_dim = HEAD_DIM // 2
    x_first = proj_f32[..., :half_dim]
    x_second = proj_f32[..., half_dim:]
    cos_b = cos_t[:, None, :]
    sin_b = sin_t[:, None, :]
    return jnp.concatenate([x_first * cos_b - x_second * sin_b, x_second * cos_b + x_first * sin_b], axis=-1).astype(jnp.bfloat16)


def causal_attention(q_heads, k_heads, v_heads):
    groups = N_HEADS // N_KV_HEADS
    n_blocks = SEQ_LEN // REF_BLOCK
    att_scale = HEAD_DIM ** -0.5
    q_grouped = q_heads.reshape(BATCH_SIZE, SEQ_LEN, N_KV_HEADS, groups, HEAD_DIM)
    k_f32 = k_heads.astype(jnp.float32)
    v_f32 = v_heads.astype(jnp.float32)
    key_pos = jnp.arange(SEQ_LEN)

    def one_block(blk_idx):
        blk_start = blk_idx * REF_BLOCK
        q_blk = lax.dynamic_slice_in_dim(q_grouped, blk_start, REF_BLOCK, axis=1).astype(jnp.float32)
        scores = jnp.einsum("bqkgd,bskd->bkgqs", q_blk, k_f32) * att_scale
        query_pos = blk_start + jnp.arange(REF_BLOCK)
        allowed = key_pos[None, :] <= query_pos[:, None]
        scores = jnp.where(allowed, scores, -1e30)
        row_max = jnp.max(scores, axis=-1, keepdims=True)
        exp_f32 = jnp.exp(scores - row_max)
        row_sum = jnp.sum(exp_f32, axis=-1)
        weighted = jnp.einsum("bkgqs,bskd->bqkgd", exp_f32.astype(jnp.bfloat16).astype(jnp.float32), v_f32)
        return (weighted / jnp.transpose(row_sum, (0, 3, 1, 2))[..., None]).astype(jnp.bfloat16)

    blocks = lax.map(one_block, jnp.arange(n_blocks))
    return jnp.moveaxis(blocks, 0, 1).reshape(BATCH_SIZE, SEQ_LEN, N_HEADS, HEAD_DIM)


def transformer_layer(hidden, cos_t, sin_t, layer_weights):
    w_query, w_key, w_value, w_out, w_up, w_down, gain_attn, gain_mlp = layer_weights
    n_rows = BATCH_SIZE * SEQ_LEN
    normed = rms_norm(hidden, gain_attn).reshape(n_rows, D_MODEL)
    q_proj = jnp.dot(normed, w_query.reshape(D_MODEL, N_HEADS * HEAD_DIM), preferred_element_type=jnp.float32)
    k_proj = jnp.dot(normed, w_key.reshape(D_MODEL, N_KV_HEADS * HEAD_DIM), preferred_element_type=jnp.float32)
    v_proj = jnp.dot(normed, w_value.reshape(D_MODEL, N_KV_HEADS * HEAD_DIM), preferred_element_type=jnp.float32)
    q_heads = apply_rope(q_proj.reshape(BATCH_SIZE, SEQ_LEN, N_HEADS, HEAD_DIM), cos_t, sin_t)
    k_heads = apply_rope(k_proj.reshape(BATCH_SIZE, SEQ_LEN, N_KV_HEADS, HEAD_DIM), cos_t, sin_t)
    v_heads = v_proj.astype(jnp.bfloat16).reshape(BATCH_SIZE, SEQ_LEN, N_KV_HEADS, HEAD_DIM)
    attn_out = causal_attention(q_heads, k_heads, v_heads)
    attn_proj = jnp.dot(attn_out.reshape(n_rows, N_HEADS * HEAD_DIM), w_out.reshape(N_HEADS * HEAD_DIM, D_MODEL), preferred_element_type=jnp.float32)
    resid_h = (hidden.reshape(n_rows, D_MODEL).astype(jnp.float32) + attn_proj).astype(jnp.bfloat16)
    normed_mlp = rms_norm(resid_h, gain_mlp)
    gelu_act = jax.nn.gelu(jnp.dot(normed_mlp, w_up, preferred_element_type=jnp.float32), approximate=True).astype(jnp.bfloat16)
    layer_out = resid_h.astype(jnp.float32) + jnp.dot(gelu_act, w_down, preferred_element_type=jnp.float32)
    return layer_out.astype(jnp.bfloat16).reshape(BATCH_SIZE, SEQ_LEN, D_MODEL)


def reference(x_in, positions, w_query, w_key, w_value, w_out, w_up, w_down, g_attn, g_mlp):
    cos_t, sin_t = rope_tables(positions)

    def layer_body(hidden, layer_weights):
        return transformer_layer(hidden, cos_t, sin_t, layer_weights), None

    stacked = (w_query, w_key, w_value, w_out, w_up, w_down, g_attn, g_mlp)
    return lax.scan(layer_body, x_in, stacked)[0]
```

```python
import functools

import jax
import jax.numpy as jnp
from jax import lax
from jax.experimental import pallas as pl
from jax.experimental.pallas import tpu as pltpu
from jax.sharding import PartitionSpec as P

ROPE_BASE = 10000.0
NORM_EPS = 1e-6
MASKED = -1e30
VMEM_LIMIT = 62 * 2**20


def norm_rows(x_f32, gain_row):
    mean_sq = jnp.mean(x_f32 * x_f32, axis=-1, keepdims=True)
    return (x_f32 * lax.rsqrt(mean_sq + NORM_EPS) * gain_row).astype(jnp.bfloat16)


def qkv_kernel(steps, sub, x_ref, wq_ref, wk_ref, wv_ref, cos_ref, sin_ref, out_ref):
    step = pl.program_id(0)
    rows = x_ref.shape[0]
    depth, hb, dh = wq_ref.shape

    def project(w_ref, rotate):
        w = w_ref[...].reshape(depth, hb * dh)
        for r in range(0, rows, sub):
            acc = jnp.dot(x_ref[r : r + sub, :], w, preferred_element_type=jnp.float32)
            if rotate:
                cos, sin = cos_ref[r : r + sub, :], sin_ref[r : r + sub, :]
                for h in range(hb):
                    u = acc[:, h * dh : (h + 1) * dh]
                    rot = u * cos + pltpu.roll(u, dh // 2, 1) * sin
                    out_ref[r : r + sub, h * dh : (h + 1) * dh] = rot.astype(jnp.bfloat16)
            else:
                out_ref[r : r + sub, :] = acc.astype(jnp.bfloat16)

    pl.when(step < steps)(lambda: project(wq_ref, True))
    pl.when((step >= steps) & (step < 2 * steps))(lambda: project(wk_ref, True))
    pl.when(step >= 2 * steps)(lambda: project(wv_ref, False))


def qkv_project(x, w_query, w_key, w_value, cos, sin, layer):
    rows, depth = x.shape
    heads, dh = w_query.shape[2:]
    hb = 8
    steps = heads // hb
    w_spec = lambda part: pl.BlockSpec(
        (None, depth, hb, dh), lambda i: (layer, 0, jnp.clip(i - part * steps, 0, steps - 1), 0)
    )
    const = lambda shape: pl.BlockSpec(shape, lambda i: (0, 0))
    return pl.pallas_call(
        functools.partial(qkv_kernel, steps, 512),
        grid=(3 * steps,),
        in_specs=[const((rows, depth)), w_spec(0), w_spec(1), w_spec(2), const((rows, dh)), const((rows, dh))],
        out_specs=pl.BlockSpec((rows, hb * dh), lambda i: (0, i)),
        out_shape=jax.ShapeDtypeStruct((rows, 3 * heads * dh), jnp.bfloat16),
        compiler_params=pltpu.CompilerParams(vmem_limit_bytes=VMEM_LIMIT),
        cost_estimate=pl.CostEstimate(
            flops=6 * rows * depth * heads * dh, bytes_accessed=6 * depth * heads * dh, transcendentals=0
        ),
        name="qkv_project",
    )(x, w_query, w_key, w_value, cos, sin)


def scores(q, k):
    return lax.dot_general(q, k, (((1,), (1,)), ((), ())), preferred_element_type=jnp.float32)


def softmax_sum(score_list, value_list, scale2):
    row_max = functools.reduce(jnp.maximum, [jnp.max(s, axis=-1, keepdims=True) for s in score_list])
    offset = row_max * scale2
    exps = [jnp.exp2(s * scale2 - offset) for s in score_list]
    row_sum = sum(jnp.sum(e, axis=-1, keepdims=True) for e in exps)
    out = sum(
        jnp.dot(e.astype(jnp.bfloat16), v, preferred_element_type=jnp.float32) for e, v in zip(exps, value_list)
    )
    return (out * (1.0 / row_sum)).astype(jnp.bfloat16)


def whole_kernel(tile, scale2, dh, q_ref, k_ref, v_ref, out_ref):
    n_tok, width = q_ref.shape
    causal = lax.broadcasted_iota(jnp.int32, (tile, tile), 1) <= lax.broadcasted_iota(jnp.int32, (tile, tile), 0)
    for c0 in range(0, width, dh):
        cols = slice(c0, c0 + dh)
        for t in range(0, n_tok, tile):
            here = slice(t, t + tile)
            q = q_ref[here, cols]
            parts = [jnp.where(causal, scores(q, k_ref[here, cols]), MASKED)]
            values = [v_ref[here, cols]]
            if t:
                parts.append(scores(q, k_ref[:t, cols]))
                values.append(v_ref[:t, cols])
            out_ref[here, cols] = softmax_sum(parts, values, scale2)


def half_kernel(tile, piece, scale2, dh, core_ref, q_ref, k_ref, v_ref, k2_ref, v2_ref, prev_ref, out_ref):
    n_tok, width = q_ref.shape
    core = core_ref[0]
    key = lax.broadcasted_iota(jnp.int32, (tile, tile), 1)
    query = lax.broadcasted_iota(jnp.int32, (tile, tile), 0)
    causal = key <= query
    causal2 = key // piece < query // piece + core
    for c0 in range(0, width, dh):
        cols = slice(c0, c0 + dh)
        for t in range(0, n_tok, tile):
            here = slice(t, t + tile)
            q = q_ref[here, cols]
            parts = [
                jnp.where(causal, scores(q, k_ref[here, cols]), MASKED),
                jnp.where(causal2, scores(q, k2_ref[here, cols]), MASKED),
            ]
            values = [v_ref[here, cols], v2_ref[here, cols]]
            if t:
                parts += [scores(q, k_ref[:t, cols]), scores(q, k2_ref[:t, cols])]
                values += [v_ref[:t, cols], v2_ref[:t, cols]]
            out_ref[here, cols] = softmax_sum(parts, values, scale2)


def attention(qkv, kv_other, core, n_whole, piece, heads, dh):
    rows = qkv.shape[0]
    n_half = rows - n_whole
    tile = 256
    scale2 = float(dh**-0.5 * 1.4426950408889634)
    group = 2
    width = group * dh
    steps = heads // group
    params = pltpu.CompilerParams(vmem_limit_bytes=VMEM_LIMIT)
    out_shape = jax.ShapeDtypeStruct((rows, heads * dh), jnp.bfloat16)
    whole = lambda part: pl.BlockSpec((n_whole, width), lambda h: (0, part * steps + h))
    out = pl.pallas_call(
        functools.partial(whole_kernel, tile, scale2, dh),
        grid=(steps,),
        in_specs=[whole(0), whole(1), whole(2)],
        out_specs=whole(0),
        out_shape=out_shape,
        compiler_params=params,
        cost_estimate=pl.CostEstimate(
            flops=8 * n_whole * n_whole * heads * dh, bytes_accessed=8 * n_whole * heads * dh, transcendentals=0
        ),
        name="attend_whole",
    )(qkv, qkv, qkv)
    skip = n_whole // n_half
    half = lambda part: pl.BlockSpec((n_half, width), lambda h: (skip, part * steps + h))
    other = lambda part: pl.BlockSpec((n_half, width), lambda h: (0, part * steps + h))
    return pl.pallas_call(
        functools.partial(half_kernel, tile, piece, scale2, dh),
        grid=(steps,),
        in_specs=[
            pl.BlockSpec(memory_space=pltpu.SMEM),
            half(0),
            half(1),
            half(2),
            other(0),
            other(1),
            pl.BlockSpec(memory_space=pl.ANY),
        ],
        out_specs=half(0),
        out_shape=out_shape,
        input_output_aliases={6: 0},
        compiler_params=params,
        cost_estimate=pl.CostEstimate(
            flops=8 * n_half * n_half * heads * dh, bytes_accessed=12 * n_half * heads * dh, transcendentals=0
        ),
        name="attend_half",
    )(core, qkv, qkv, qkv, kv_other, kv_other, out)


def out_kernel(sub, o_ref, x_ref, w_ref, g_ref, h_ref, r_ref):
    for r in range(0, o_ref.shape[0], sub):
        prod = jnp.dot(o_ref[r : r + sub, :], w_ref[...], preferred_element_type=jnp.float32)
        h = (x_ref[r : r + sub, :].astype(jnp.float32) + prod).astype(jnp.bfloat16)
        h_ref[r : r + sub, :] = h
        r_ref[r : r + sub, :] = norm_rows(h.astype(jnp.float32), g_ref[...])


def out_project(o, x, w_out, gain, layer):
    rows, depth = o.shape
    width = x.shape[1]
    mb = 512
    row_spec = lambda n: pl.BlockSpec((mb, n), lambda m: (m, 0))
    return pl.pallas_call(
        functools.partial(out_kernel, 256),
        grid=(rows // mb,),
        in_specs=[
            row_spec(depth),
            row_spec(width),
            pl.BlockSpec((None, depth, width), lambda m: (layer, 0, 0), pipeline_mode=pl.Buffered(1)),
            pl.BlockSpec((1, width), lambda m: (0, 0)),
        ],
        out_specs=[row_spec(width)] * 2,
        out_shape=[jax.ShapeDtypeStruct((rows, width), jnp.bfloat16)] * 2,
        compiler_params=pltpu.CompilerParams(vmem_limit_bytes=VMEM_LIMIT),
        cost_estimate=pl.CostEstimate(
            flops=2 * rows * depth * width, bytes_accessed=2 * depth * width, transcendentals=0
        ),
        name="out_project",
    )(o, x, w_out, gain)


def mlp_kernel(sub, r_ref, h_ref, up_ref, down_ref, g_ref, y_ref, n_ref, acc):
    f = pl.program_id(1)
    rows = r_ref.shape[0]

    @pl.when(f == 0)
    def _():
        acc[...] = jnp.zeros_like(acc)

    for r in range(0, rows, sub):
        u = jnp.dot(r_ref[r : r + sub, :], up_ref[...], preferred_element_type=jnp.float32)
        z = jax.nn.gelu(u, approximate=True).astype(jnp.bfloat16)
        acc[r : r + sub, :] += jnp.dot(z, down_ref[...], preferred_element_type=jnp.float32)

    @pl.when(f == pl.num_programs(1) - 1)
    def _():
        for r in range(0, rows, 256):
            y = (h_ref[r : r + 256, :].astype(jnp.float32) + acc[r : r + 256, :]).astype(jnp.bfloat16)
            y_ref[r : r + 256, :] = y
            n_ref[r : r + 256, :] = norm_rows(y.astype(jnp.float32), g_ref[...])


def mlp(r, h, w_up, w_down, gain, layer):
    rows, width = r.shape
    ff = w_up.shape[2]
    mb, tf, sub = 768, 1024, 384
    row_spec = pl.BlockSpec((mb, width), lambda m, f: (m, 0))
    return pl.pallas_call(
        functools.partial(mlp_kernel, sub),
        grid=(rows // mb, ff // tf),
        in_specs=[
            row_spec,
            row_spec,
            pl.BlockSpec((None, width, tf), lambda m, f: (layer, 0, f)),
            pl.BlockSpec((None, tf, width), lambda m, f: (layer, f, 0)),
            pl.BlockSpec((1, width), lambda m, f: (0, 0)),
        ],
        out_specs=[row_spec] * 2,
        out_shape=[jax.ShapeDtypeStruct((rows, width), jnp.bfloat16)] * 2,
        scratch_shapes=[pltpu.VMEM((mb, width), jnp.float32)],
        compiler_params=pltpu.CompilerParams(vmem_limit_bytes=VMEM_LIMIT),
        cost_estimate=pl.CostEstimate(
            flops=4 * rows * ff * width, bytes_accessed=4 * ff * width, transcendentals=0
        ),
        name="mlp",
    )(r, h, w_up, w_down, gain)


def solution(mesh):
    n_seq = mesh.shape["seq"]
    n_pair = n_seq // 2
    tok_spec = P(None, ("data", "seq"), None)
    in_specs = (tok_spec, P(("data", "seq"))) + (P(),) * 8
    partner = [(i, i ^ 1) for i in range(n_seq)]

    def device_fn(x_loc, pos_loc, w_query, w_key, w_value, w_out, w_up, w_down, g_attn, g_mlp):
        n_layers, _, heads, dh = w_query.shape
        n_batch, shard, width = x_loc.shape
        per = n_batch // n_pair
        assert per * n_pair == n_batch and per == 3
        piece = shard // 2
        core = lax.rem(lax.axis_index("seq"), 2)
        exchange = lambda a: lax.all_to_all(a, "seq", 0, 0, tiled=True)

        by_chip = x_loc.reshape(n_pair, per, shard, width)
        whole = exchange(by_chip[:, :2].reshape(n_seq, shard, width))
        half = exchange(by_chip[:, 2].reshape(n_seq, piece, width))
        hidden = jnp.concatenate([whole.reshape(n_seq * shard, width), half.reshape(n_seq * piece, width)])
        n_whole = n_seq * shard

        pos = lax.all_gather(pos_loc, "seq", tiled=True)
        pos_half = lax.dynamic_index_in_dim(pos.reshape(n_seq, 2, piece), core, axis=1, keepdims=False).reshape(-1)
        inv_freq = ROPE_BASE ** (-jnp.arange(dh // 2, dtype=jnp.float32) * (2.0 / dh))
        angles = jnp.concatenate([pos, pos_half]).astype(jnp.float32)[:, None] * inv_freq
        cos, sin = jnp.cos(angles), jnp.sin(angles)
        cos = jnp.concatenate([cos, cos], axis=-1)
        sin = jnp.concatenate([-sin, sin], axis=-1)
        core_arr = core.astype(jnp.int32).reshape(1)
        w_out2 = w_out.reshape(n_layers, heads * dh, width)

        normed = norm_rows(hidden.astype(jnp.float32), g_attn[0])
        for layer in range(n_layers):
            qkv = qkv_project(normed, w_query, w_key, w_value, cos, sin, layer)
            kv_other = lax.ppermute(qkv[n_whole:, heads * dh :], "seq", partner)
            attn = attention(qkv, kv_other, core_arr, n_whole, piece, heads, dh)
            resid, r = out_project(attn, hidden, w_out2, g_mlp[layer][None], layer)
            following = g_attn[min(layer + 1, n_layers - 1)][None]
            hidden, normed = mlp(r, resid, w_up, w_down, following, layer)

        whole = exchange(hidden[:n_whole].reshape(n_seq, shard, width)).reshape(n_pair, 2, shard, width)
        half = exchange(hidden[n_whole:].reshape(n_seq, piece, width)).reshape(n_pair, 1, shard, width)
        return jnp.concatenate([whole, half], axis=1).reshape(n_batch, shard, width)

    return jax.shard_map(device_fn, mesh=mesh, in_specs=in_specs, out_specs=tok_spec, check_vma=False)
```

```python
import functools

import jax
import jax.numpy as jnp
from jax import lax
from jax.experimental import pallas as pl
from jax.experimental.pallas import tpu as pltpu
from jax.sharding import PartitionSpec as P

ROPE_BASE = 10000.0
NORM_EPS = 1e-6
MASKED = -1e30
VMEM_LIMIT = 62 * 2**20


def norm_rows(x_f32, gain_row):
    mean_sq = jnp.mean(x_f32 * x_f32, axis=-1, keepdims=True)
    return (x_f32 * lax.rsqrt(mean_sq + NORM_EPS) * gain_row).astype(jnp.bfloat16)


def flat(ref, lo, n):
    return ref[lo : lo + n].reshape(n * ref.shape[1], ref.shape[2])


def project_steps(steps, group, get_x, wq_ref, wk_ref, wv_ref, cos_ref, sin_ref, out_ref, kv_ref, kv_lo):
    step = pl.program_id(0)
    groups, per_group = out_ref.shape[:2]
    depth, hb, dh = wq_ref.shape

    def project(w_ref, rotate, keep):
        w = w_ref[...].reshape(depth, hb * dh)
        for lo in range(0, groups, group):
            here = slice(lo, lo + group)
            acc = jnp.dot(get_x(lo, group), w, preferred_element_type=jnp.float32)
            if rotate:
                cos, sin = flat(cos_ref, lo, group), flat(sin_ref, lo, group)
                for h in range(hb):
                    cols = slice(h * dh, (h + 1) * dh)
                    u = acc[:, cols]
                    rot = (u * cos + pltpu.roll(u, dh // 2, 1) * sin).astype(jnp.bfloat16)
                    out_ref[here, :, cols] = rot.reshape(group, per_group, dh)
            else:
                out_ref[here] = acc.astype(jnp.bfloat16).reshape(group, per_group, hb * dh)
        if keep and kv_ref is not None:
            kv_ref[...] = out_ref[:, kv_lo:, :]

    pl.when(step < steps)(lambda: project(wq_ref, True, False))
    pl.when((step >= steps) & (step < 2 * steps))(lambda: project(wk_ref, True, True))
    pl.when(step >= 2 * steps)(lambda: project(wv_ref, False, True))


def later_kernel(steps, group, kv_lo, x_ref, wq_ref, wk_ref, wv_ref, cos_ref, sin_ref, out_ref, kv_ref):
    get_x = lambda lo, n: flat(x_ref, lo, n)
    project_steps(steps, group, get_x, wq_ref, wk_ref, wv_ref, cos_ref, sin_ref, out_ref, kv_ref, kv_lo)


def first_kernel(steps, with_kv, n_prev, x_ref, g_ref, wq_ref, wk_ref, wv_ref, cos_ref, sin_ref, *refs):
    out_ref, hid_ref = refs[n_prev : n_prev + 2]
    kv_ref = refs[n_prev + 2] if with_kv else None
    xn_ref = refs[-1]

    @pl.when(pl.program_id(0) == 0)
    def _():
        x = x_ref[...]
        hid_ref[...] = x
        xn_ref[...] = norm_rows(x.reshape(xn_ref.shape).astype(jnp.float32), g_ref[...])

    get_x = lambda lo, n: xn_ref[...]
    project_steps(steps, x_ref.shape[0], get_x, wq_ref, wk_ref, wv_ref, cos_ref, sin_ref, out_ref, kv_ref, 0)


def weight_specs(w, layer, hb):
    depth, heads, dh = w.shape[1:]
    steps = heads // hb
    pick = lambda part: pl.BlockSpec(
        (None, depth, hb, dh), lambda i: (layer, 0, jnp.clip(i - part * steps, 0, steps - 1), 0)
    )
    return [pick(0), pick(1), pick(2)], steps


def qkv_cost(rows, w):
    n = w.shape[1] * w.shape[2] * w.shape[3]
    return pl.CostEstimate(flops=6 * rows * n, bytes_accessed=6 * n, transcendentals=0)


def qkv_first(x_part, part, prev, w_query, w_key, w_value, cos, sin, gain, with_kv):
    shards, piece, depth = x_part.shape
    per_shard = cos.shape[1]
    heads, dh = w_query.shape[2:]
    hb = 8
    w_specs, steps = weight_specs(w_query, 0, hb)
    kv_block = lambda i: (0, 0, jnp.clip(i - steps, 0, 2 * steps - 1))
    whole = lambda shape: pl.BlockSpec(shape, lambda i: (0,) * len(shape))
    here = lambda n: pl.BlockSpec((shards, piece, n), lambda i: (0, part, 0))
    out_specs = [pl.BlockSpec((shards, piece, hb * dh), lambda i: (0, part, i)), here(depth)]
    out_shape = [
        jax.ShapeDtypeStruct((shards, per_shard, 3 * heads * dh), jnp.bfloat16),
        jax.ShapeDtypeStruct((shards, per_shard, depth), jnp.bfloat16),
    ]
    if with_kv:
        out_specs.append(pl.BlockSpec((shards, piece, hb * dh), kv_block))
        out_shape.append(jax.ShapeDtypeStruct((shards, piece, 2 * heads * dh), jnp.bfloat16))
    return pl.pallas_call(
        functools.partial(first_kernel, steps, with_kv, len(prev)),
        grid=(3 * steps,),
        in_specs=[whole((shards, piece, depth)), whole((1, depth)), *w_specs, here(dh), here(dh)]
        + [pl.BlockSpec(memory_space=pl.ANY)] * len(prev),
        out_specs=out_specs,
        out_shape=out_shape,
        input_output_aliases={7 + i: i for i in range(len(prev))},
        scratch_shapes=[pltpu.VMEM((shards * piece, depth), jnp.bfloat16)],
        compiler_params=pltpu.CompilerParams(vmem_limit_bytes=VMEM_LIMIT),
        cost_estimate=qkv_cost(shards * piece, w_query),
        name="qkv_first",
    )(x_part, gain, w_query, w_key, w_value, cos, sin, *prev)


def qkv_later(x, w_query, w_key, w_value, cos, sin, layer, piece):
    shards, per_shard, depth = x.shape
    heads, dh = w_query.shape[2:]
    hb = 8
    w_specs, steps = weight_specs(w_query, layer, hb)
    kv_block = lambda i: (0, 0, jnp.clip(i - steps, 0, 2 * steps - 1))
    whole = lambda shape: pl.BlockSpec(shape, lambda i: (0,) * len(shape))
    return pl.pallas_call(
        functools.partial(later_kernel, steps, shards // 2, per_shard - piece),
        grid=(3 * steps,),
        in_specs=[whole(x.shape), *w_specs, whole(cos.shape), whole(sin.shape)],
        out_specs=[
            pl.BlockSpec((shards, per_shard, hb * dh), lambda i: (0, 0, i)),
            pl.BlockSpec((shards, piece, hb * dh), kv_block),
        ],
        out_shape=[
            jax.ShapeDtypeStruct((shards, per_shard, 3 * heads * dh), jnp.bfloat16),
            jax.ShapeDtypeStruct((shards, piece, 2 * heads * dh), jnp.bfloat16),
        ],
        compiler_params=pltpu.CompilerParams(vmem_limit_bytes=VMEM_LIMIT),
        cost_estimate=qkv_cost(shards * per_shard, w_query),
        name="qkv_later",
    )(x, w_query, w_key, w_value, cos, sin)


def scores(q, k):
    return lax.dot_general(q, k, (((1,), (1,)), ((), ())), preferred_element_type=jnp.float32)


def softmax_sum(score_list, value_list, scale2):
    row_max = functools.reduce(jnp.maximum, [jnp.max(s, axis=-1, keepdims=True) for s in score_list])
    offset = row_max * scale2
    exps = [jnp.exp2(s * scale2 - offset) for s in score_list]
    row_sum = sum(jnp.sum(e, axis=-1, keepdims=True) for e in exps)
    out = sum(
        jnp.dot(e.astype(jnp.bfloat16), v, preferred_element_type=jnp.float32) for e, v in zip(exps, value_list)
    )
    return (out * (1.0 / row_sum)).astype(jnp.bfloat16)


def run_tiles(n_heads, n_tiles, get_scores, finish):
    order = [(h, t if h % 2 == 0 else n_tiles - 1 - t) for h in range(n_heads) for t in range(n_tiles)]
    held = get_scores(*order[0])
    for pos, task in enumerate(order):
        ahead = get_scores(*order[pos + 1]) if pos + 1 < len(order) else None
        finish(*task, held)
        held = ahead


def whole_kernel(tile, scale2, dh, q_ref, k_ref, v_ref, out_ref):
    shards, per, width = q_ref.shape
    gt = tile // per
    causal = lax.broadcasted_iota(jnp.int32, (tile, tile), 1) <= lax.broadcasted_iota(jnp.int32, (tile, tile), 0)
    part = lambda ref, lo, n, h: ref[lo : lo + n, :, h * dh : (h + 1) * dh].reshape(n * per, dh)

    def get_scores(h, t):
        q = part(q_ref, t * gt, gt, h)
        s = scores(q, part(k_ref, 0, (t + 1) * gt, h))
        last = jnp.where(causal, s[:, t * tile :], MASKED)
        return [s[:, : t * tile], last] if t else [last]

    def finish(h, t, held):
        values = [part(v_ref, 0, t * gt, h)] if t else []
        values.append(part(v_ref, t * gt, gt, h))
        out = softmax_sum(held, values, scale2)
        out_ref[t * gt : (t + 1) * gt, :, h * dh : (h + 1) * dh] = out.reshape(gt, per, dh)

    run_tiles(width // dh, shards // gt, get_scores, finish)


def half_kernel(tile, scale2, dh, core_ref, q_ref, k_ref, v_ref, k2_ref, v2_ref, prev_ref, out_ref):
    shards, piece, width = q_ref.shape
    gt = tile // piece
    core = core_ref[0]
    key = lax.broadcasted_iota(jnp.int32, (tile, tile), 1)
    query = lax.broadcasted_iota(jnp.int32, (tile, tile), 0)
    causal = key <= query
    causal2 = key // piece < query // piece + core
    part = lambda ref, lo, n, h: ref[lo : lo + n, :, h * dh : (h + 1) * dh].reshape(n * piece, dh)

    def get_scores(h, t):
        q = part(q_ref, t * gt, gt, h)
        out = []
        for ref, mask in ((k_ref, causal), (k2_ref, causal2)):
            s = scores(q, part(ref, 0, (t + 1) * gt, h))
            out += [s[:, : t * tile]] if t else []
            out.append(jnp.where(mask, s[:, t * tile :], MASKED))
        return out

    def finish(h, t, held):
        values = []
        for ref in (v_ref, v2_ref):
            values += [part(ref, 0, t * gt, h)] if t else []
            values.append(part(ref, t * gt, gt, h))
        out = softmax_sum(held, values, scale2)
        out_ref[t * gt : (t + 1) * gt, :, h * dh : (h + 1) * dh] = out.reshape(gt, piece, dh)

    run_tiles(width // dh, shards // gt, get_scores, finish)


def attention(qkv, kv_own, kv_other, core, heads, dh):
    shards, per_shard = qkv.shape[:2]
    piece = kv_own.shape[1]
    n_whole, n_half = shards * 2 * piece, shards * piece
    tile = 256
    scale2 = float(dh**-0.5 * 1.4426950408889634)
    group = 2
    width = group * dh
    steps = heads // group
    params = pltpu.CompilerParams(vmem_limit_bytes=VMEM_LIMIT)
    out_shape = jax.ShapeDtypeStruct((shards, per_shard, heads * dh), jnp.bfloat16)
    whole = lambda third: pl.BlockSpec((shards, 2 * piece, width), lambda h: (0, 0, third * steps + h))
    out = pl.pallas_call(
        functools.partial(whole_kernel, tile, scale2, dh),
        grid=(steps,),
        in_specs=[whole(0), whole(1), whole(2)],
        out_specs=whole(0),
        out_shape=out_shape,
        compiler_params=params,
        cost_estimate=pl.CostEstimate(
            flops=8 * n_whole * n_whole * heads * dh, bytes_accessed=8 * n_whole * heads * dh, transcendentals=0
        ),
        name="attend_whole",
    )(qkv, qkv, qkv)
    shared = pl.BlockSpec((shards, piece, width), lambda h: (0, 2, h))
    side = lambda second: pl.BlockSpec((shards, piece, width), lambda h: (0, 0, second * steps + h))
    return pl.pallas_call(
        functools.partial(half_kernel, tile, scale2, dh),
        grid=(steps,),
        in_specs=[
            pl.BlockSpec(memory_space=pltpu.SMEM),
            shared,
            side(0),
            side(1),
            side(0),
            side(1),
            pl.BlockSpec(memory_space=pl.ANY),
        ],
        out_specs=shared,
        out_shape=out_shape,
        input_output_aliases={6: 0},
        compiler_params=params,
        cost_estimate=pl.CostEstimate(
            flops=8 * n_half * n_half * heads * dh, bytes_accessed=12 * n_half * heads * dh, transcendentals=0
        ),
        name="attend_half",
    )(core, qkv, kv_own, kv_own, kv_other, kv_other, out)


def out_kernel(sub, o_ref, x_ref, w_ref, g_ref, h_ref, r_ref, acc):
    k, m = pl.program_id(0), pl.program_id(1)
    last = pl.num_programs(0) - 1
    rows = o_ref.shape[0]
    dot = lambda r: jnp.dot(o_ref[r : r + sub, :], w_ref[...], preferred_element_type=jnp.float32)

    @pl.when(k == 0)
    def _():
        for r in range(0, rows, sub):
            acc[m, r : r + sub, :] = dot(r)

    @pl.when((k > 0) & (k < last))
    def _():
        for r in range(0, rows, sub):
            acc[m, r : r + sub, :] += dot(r)

    @pl.when(k == last)
    def _():
        held = dot(0)
        for r in range(0, rows, sub):
            ahead = dot(r + sub) if r + sub < rows else None
            h = (x_ref[r : r + sub, :].astype(jnp.float32) + (acc[m, r : r + sub, :] + held)).astype(jnp.bfloat16)
            h_ref[r : r + sub, :] = h
            r_ref[r : r + sub, :] = norm_rows(h.astype(jnp.float32), g_ref[...])
            held = ahead


def out_project(o, x, w_out, gain, layer):
    rows, depth = o.shape
    width = x.shape[1]
    mb, tk = 512, depth // 2
    at_end = pl.BlockSpec((mb, width), lambda k, m: (jnp.where(k == depth // tk - 1, m, 0), 0))
    return pl.pallas_call(
        functools.partial(out_kernel, 256),
        grid=(depth // tk, rows // mb),
        in_specs=[
            pl.BlockSpec((mb, tk), lambda k, m: (m, k)),
            at_end,
            pl.BlockSpec((None, tk, width), lambda k, m: (layer, k, 0)),
            pl.BlockSpec((1, width), lambda k, m: (0, 0)),
        ],
        out_specs=[at_end] * 2,
        out_shape=[jax.ShapeDtypeStruct((rows, width), jnp.bfloat16)] * 2,
        scratch_shapes=[pltpu.VMEM((rows // mb, mb, width), jnp.float32)],
        compiler_params=pltpu.CompilerParams(vmem_limit_bytes=VMEM_LIMIT),
        cost_estimate=pl.CostEstimate(
            flops=2 * rows * depth * width, bytes_accessed=2 * depth * width, transcendentals=0
        ),
        name="out_project",
    )(o, x, w_out, gain)


def mlp_kernel(group, r_ref, h_ref, up_ref, down_ref, *refs):
    g_ref, y_ref, n_ref, acc = refs if len(refs) == 4 else (None, refs[0], None, refs[1])
    f = pl.program_id(1)
    groups, per, width = r_ref.shape
    sub = group * per
    up = lambda lo: jnp.dot(flat(r_ref, lo, group), up_ref[...], preferred_element_type=jnp.float32)

    def add_block(first):
        held = up(0)
        for lo in range(0, groups, group):
            ahead = up(lo + group) if lo + group < groups else None
            z = jax.nn.gelu(held, approximate=True).astype(jnp.bfloat16)
            prod = jnp.dot(z, down_ref[...], preferred_element_type=jnp.float32)
            rows = slice(lo * per, lo * per + sub)
            if first:
                acc[rows, :] = prod
            else:
                acc[rows, :] += prod
            held = ahead

    pl.when(f == 0)(lambda: add_block(True))
    pl.when(f > 0)(lambda: add_block(False))

    @pl.when(f == pl.num_programs(1) - 1)
    def _():
        for lo in range(groups):
            rows = slice(lo * per, (lo + 1) * per)
            y = (h_ref[lo].astype(jnp.float32) + acc[rows, :]).astype(jnp.bfloat16)
            y_ref[lo] = y
            if n_ref is not None:
                n_ref[lo] = norm_rows(y.astype(jnp.float32), g_ref[...])


def mlp(r, h, w_up, w_down, gain, layer, part=None, piece=None):
    shards, per_shard, width = r.shape
    ff = w_up.shape[2]
    tf = 1024
    if part is None:
        blocks, block = 2, (shards // 2, per_shard, width)
        group = shards // 4
        in_row = out_row = pl.BlockSpec(block, lambda m, f: (m, 0, 0))
        extra, extra_specs = [gain], [pl.BlockSpec((1, width), lambda m, f: (0, 0))]
        out_shape = [jax.ShapeDtypeStruct(r.shape, jnp.bfloat16)] * 2
    else:
        blocks, block = 1, (shards, piece, width)
        group = shards // 2
        in_row = pl.BlockSpec(block, lambda m, f: (0, part, 0))
        out_row = pl.BlockSpec(block, lambda m, f: (0, 0, 0))
        extra, extra_specs = [], []
        out_shape = [jax.ShapeDtypeStruct(block, jnp.bfloat16)]
    rows = blocks * block[0] * block[1]
    return pl.pallas_call(
        functools.partial(mlp_kernel, group),
        grid=(blocks, ff // tf),
        in_specs=[
            in_row,
            in_row,
            pl.BlockSpec((None, width, tf), lambda m, f: (layer, 0, f)),
            pl.BlockSpec((None, tf, width), lambda m, f: (layer, f, 0)),
            *extra_specs,
        ],
        out_specs=[out_row] * len(out_shape),
        out_shape=out_shape,
        scratch_shapes=[pltpu.VMEM((block[0] * block[1], width), jnp.float32)],
        compiler_params=pltpu.CompilerParams(vmem_limit_bytes=VMEM_LIMIT),
        cost_estimate=pl.CostEstimate(
            flops=4 * rows * ff * width, bytes_accessed=4 * ff * width, transcendentals=0
        ),
        name="mlp",
    )(r, h, w_up, w_down, *extra)


def solution(mesh):
    n_seq = mesh.shape["seq"]
    n_pair = n_seq // 2
    tok_spec = P(None, ("data", "seq"), None)
    in_specs = (tok_spec, P(("data", "seq"))) + (P(),) * 8
    partner = [(i, i ^ 1) for i in range(n_seq)]

    def device_fn(x_loc, pos_loc, w_query, w_key, w_value, w_out, w_up, w_down, g_attn, g_mlp):
        n_layers, _, heads, dh = w_query.shape
        n_batch, shard, width = x_loc.shape
        per = n_batch // n_pair
        assert per * n_pair == n_batch and per == 3
        piece = shard // 2
        core = lax.rem(lax.axis_index("seq"), 2)
        exchange = lambda a: lax.all_to_all(a, "seq", 0, 0, tiled=True)

        pos = lax.all_gather(pos_loc, "seq", tiled=True).reshape(n_seq, shard)
        by_chip = x_loc.reshape(n_pair, per, shard, width)
        sends = [by_chip[:, :2, i * piece : (i + 1) * piece].reshape(n_seq, piece, width) for i in range(2)]
        first, pos = lax.optimization_barrier((by_chip[:, 2].reshape(n_seq, piece, width), pos))
        shared_x = exchange(first)
        shared_x, send0 = lax.optimization_barrier((shared_x, sends[0]))
        x0 = exchange(send0)
        x0, send1 = lax.optimization_barrier((x0, sends[1]))
        x1 = exchange(send1)

        pos_shared = lax.dynamic_index_in_dim(pos.reshape(n_seq, 2, piece), core, axis=1, keepdims=False)
        inv_freq = ROPE_BASE ** (-jnp.arange(dh // 2, dtype=jnp.float32) * (2.0 / dh))
        angles = jnp.concatenate([pos, pos_shared], axis=1).astype(jnp.float32)[..., None] * inv_freq
        cos, sin = jnp.cos(angles), jnp.sin(angles)
        cos = jnp.concatenate([cos, cos], axis=-1)
        sin = jnp.concatenate([-sin, sin], axis=-1)
        core_arr = core.astype(jnp.int32).reshape(1)
        w_out2 = w_out.reshape(n_layers, heads * dh, width)
        flat2 = lambda a: a.reshape(-1, a.shape[-1])

        first_args = (w_query, w_key, w_value, cos, sin, g_attn[0][None])
        qkv, hidden, kv_own = qkv_first(shared_x, 2, [], *first_args, True)
        qkv, hidden = qkv_first(x0, 0, [qkv, hidden], *first_args, False)
        qkv, hidden = qkv_first(x1, 1, [qkv, hidden], *first_args, False)
        for layer in range(n_layers):
            if layer:
                qkv, kv_own = qkv_later(normed, w_query, w_key, w_value, cos, sin, layer, piece)
            kv_other = lax.ppermute(kv_own, "seq", partner)
            attn = attention(qkv, kv_own, kv_other, core_arr, heads, dh)
            resid, r = out_project(flat2(attn), flat2(hidden), w_out2, g_mlp[layer][None], layer)
            resid, r = resid.reshape(hidden.shape), r.reshape(hidden.shape)
            if layer < n_layers - 1:
                hidden, normed = mlp(r, resid, w_up, w_down, g_attn[layer + 1][None], layer)

        parts = []
        for part in range(3):
            (y,) = mlp(r, resid, w_up, w_down, None, n_layers - 1, part, piece)
            parts.append(exchange(y))
        whole = jnp.concatenate([a.reshape(n_pair, 2, piece, width) for a in parts[:2]], axis=2)
        shared = parts[2].reshape(n_pair, 1, shard, width)
        return jnp.concatenate([whole, shared], axis=1).reshape(n_batch, shard, width)

    return jax.shard_map(device_fn, mesh=mesh, in_specs=in_specs, out_specs=tok_spec, check_vma=False)
```

```python
import functools

import jax
import jax.numpy as jnp
from jax import lax
from jax.experimental import pallas as pl
from jax.experimental.pallas import tpu as pltpu
from jax.sharding import PartitionSpec as P


ROPE_BASE = 10000.0
NORM_EPS = 1e-6
MASKED = -1e30
VMEM_LIMIT = 62 * 2**20


def norm_rows(x_f32, gain_row):
    mean_sq = jnp.mean(x_f32 * x_f32, axis=-1, keepdims=True)
    return (x_f32 * lax.rsqrt(mean_sq + NORM_EPS) * gain_row).astype(jnp.bfloat16)


def flat(ref, lo, n):
    return ref[lo : lo + n].reshape(n * ref.shape[1], ref.shape[2])


def project_steps(steps, group, get_x, wq_ref, wk_ref, wv_ref, cos_ref, sin_ref, out_ref, kv_ref, kv_lo):
    step = pl.program_id(0)
    groups, per_group = out_ref.shape[:2]
    depth, hb, dh = wq_ref.shape

    def project(w_ref, rotate, keep):
        w = w_ref[...].reshape(depth, hb * dh)
        for lo in range(0, groups, group):
            here = slice(lo, lo + group)
            acc = jnp.dot(get_x(lo, group), w, preferred_element_type=jnp.float32)
            if rotate:
                cos, sin = flat(cos_ref, lo, group), flat(sin_ref, lo, group)
                for h in range(hb):
                    cols = slice(h * dh, (h + 1) * dh)
                    u = acc[:, cols]
                    rot = (u * cos + pltpu.roll(u, dh // 2, 1) * sin).astype(jnp.bfloat16)
                    out_ref[here, :, cols] = rot.reshape(group, per_group, dh)
            else:
                out_ref[here] = acc.astype(jnp.bfloat16).reshape(group, per_group, hb * dh)
        if keep and kv_ref is not None:
            kv_ref[...] = out_ref[:, kv_lo:, :]

    pl.when(step < steps)(lambda: project(wq_ref, True, False))
    pl.when((step >= steps) & (step < 2 * steps))(lambda: project(wk_ref, True, True))
    pl.when(step >= 2 * steps)(lambda: project(wv_ref, False, True))


def later_kernel(steps, group, kv_lo, x_ref, wq_ref, wk_ref, wv_ref, cos_ref, sin_ref, out_ref, kv_ref):
    get_x = lambda lo, n: flat(x_ref, lo, n)
    project_steps(steps, group, get_x, wq_ref, wk_ref, wv_ref, cos_ref, sin_ref, out_ref, kv_ref, kv_lo)


def first_kernel(steps, with_kv, n_prev, x_ref, g_ref, wq_ref, wk_ref, wv_ref, cos_ref, sin_ref, *refs):
    out_ref, hid_ref = refs[n_prev : n_prev + 2]
    kv_ref = refs[n_prev + 2] if with_kv else None
    xn_ref = refs[-1]

    @pl.when(pl.program_id(0) == 0)
    def _():
        x = x_ref[...]
        hid_ref[...] = x
        xn_ref[...] = norm_rows(x.reshape(xn_ref.shape).astype(jnp.float32), g_ref[...])

    get_x = lambda lo, n: xn_ref[...]
    project_steps(steps, x_ref.shape[0], get_x, wq_ref, wk_ref, wv_ref, cos_ref, sin_ref, out_ref, kv_ref, 0)


def weight_specs(w, layer, hb):
    depth, heads, dh = w.shape[1:]
    steps = heads // hb
    pick = lambda part: pl.BlockSpec(
        (None, depth, hb, dh), lambda i: (layer, 0, jnp.clip(i - part * steps, 0, steps - 1), 0)
    )
    return [pick(0), pick(1), pick(2)], steps


def qkv_cost(rows, w):
    n = w.shape[1] * w.shape[2] * w.shape[3]
    return pl.CostEstimate(flops=6 * rows * n, bytes_accessed=6 * n, transcendentals=0)


def qkv_first(x_part, part, prev, w_query, w_key, w_value, cos, sin, gain, with_kv):
    shards, piece, depth = x_part.shape
    per_shard = cos.shape[1]
    heads, dh = w_query.shape[2:]
    hb = 8
    w_specs, steps = weight_specs(w_query, 0, hb)
    kv_block = lambda i: (0, 0, jnp.clip(i - steps, 0, 2 * steps - 1))
    whole = lambda shape: pl.BlockSpec(shape, lambda i: (0,) * len(shape))
    here = lambda n: pl.BlockSpec((shards, piece, n), lambda i: (0, part, 0))
    out_specs = [pl.BlockSpec((shards, piece, hb * dh), lambda i: (0, part, i)), here(depth)]
    out_shape = [
        jax.ShapeDtypeStruct((shards, per_shard, 3 * heads * dh), jnp.bfloat16),
        jax.ShapeDtypeStruct((shards, per_shard, depth), jnp.bfloat16),
    ]
    if with_kv:
        out_specs.append(pl.BlockSpec((shards, piece, hb * dh), kv_block))
        out_shape.append(jax.ShapeDtypeStruct((shards, piece, 2 * heads * dh), jnp.bfloat16))
    return pl.pallas_call(
        functools.partial(first_kernel, steps, with_kv, len(prev)),
        grid=(3 * steps,),
        in_specs=[whole((shards, piece, depth)), whole((1, depth)), *w_specs, here(dh), here(dh)]
        + [pl.BlockSpec(memory_space=pl.ANY)] * len(prev),
        out_specs=out_specs,
        out_shape=out_shape,
        input_output_aliases={7 + i: i for i in range(len(prev))},
        scratch_shapes=[pltpu.VMEM((shards * piece, depth), jnp.bfloat16)],
        compiler_params=pltpu.CompilerParams(vmem_limit_bytes=VMEM_LIMIT),
        cost_estimate=qkv_cost(shards * piece, w_query),
        name="qkv_first",
    )(x_part, gain, w_query, w_key, w_value, cos, sin, *prev)


def qkv_later(x, w_query, w_key, w_value, cos, sin, layer, piece):
    shards, per_shard, _ = x.shape
    heads, dh = w_query.shape[2:]
    hb = 8
    w_specs, steps = weight_specs(w_query, layer, hb)
    kv_block = lambda i: (0, 0, jnp.clip(i - steps, 0, 2 * steps - 1))
    whole = lambda shape: pl.BlockSpec(shape, lambda i: (0,) * len(shape))
    return pl.pallas_call(
        functools.partial(later_kernel, steps, shards // 2, per_shard - piece),
        grid=(3 * steps,),
        in_specs=[whole(x.shape), *w_specs, whole(cos.shape), whole(sin.shape)],
        out_specs=[
            pl.BlockSpec((shards, per_shard, hb * dh), lambda i: (0, 0, i)),
            pl.BlockSpec((shards, piece, hb * dh), kv_block),
        ],
        out_shape=[
            jax.ShapeDtypeStruct((shards, per_shard, 3 * heads * dh), jnp.bfloat16),
            jax.ShapeDtypeStruct((shards, piece, 2 * heads * dh), jnp.bfloat16),
        ],
        compiler_params=pltpu.CompilerParams(vmem_limit_bytes=VMEM_LIMIT),
        cost_estimate=qkv_cost(shards * per_shard, w_query),
        name="qkv_later",
    )(x, w_query, w_key, w_value, cos, sin)


def scores(q, k):
    return lax.dot_general(q, k, (((1,), (1,)), ((), ())), preferred_element_type=jnp.float32)


def softmax_sum(score_list, value_list, scale2):
    row_max = functools.reduce(jnp.maximum, [jnp.max(s, axis=-1, keepdims=True) for s in score_list])
    offset = row_max * scale2
    exps = [jnp.exp2(s * scale2 - offset) for s in score_list]
    row_sum = sum(jnp.sum(e, axis=-1, keepdims=True) for e in exps)
    out = sum(
        jnp.dot(e.astype(jnp.bfloat16), v, preferred_element_type=jnp.float32) for e, v in zip(exps, value_list)
    )
    return (out * (1.0 / row_sum)).astype(jnp.bfloat16)


def run_tiles(n_heads, n_tiles, get_scores, finish):
    order = [(h, t if h % 2 == 0 else n_tiles - 1 - t) for h in range(n_heads) for t in range(n_tiles)]
    held = get_scores(*order[0])
    for pos, task in enumerate(order):
        ahead = get_scores(*order[pos + 1]) if pos + 1 < len(order) else None
        finish(*task, held)
        held = ahead


def whole_kernel(tile, scale2, dh, q_ref, k_ref, v_ref, out_ref):
    shards, per, width = q_ref.shape
    gt = tile // per
    causal = lax.broadcasted_iota(jnp.int32, (tile, tile), 1) <= lax.broadcasted_iota(jnp.int32, (tile, tile), 0)
    part = lambda ref, lo, n, h: ref[lo : lo + n, :, h * dh : (h + 1) * dh].reshape(n * per, dh)

    def get_scores(h, t):
        q = part(q_ref, t * gt, gt, h)
        s = scores(q, part(k_ref, 0, (t + 1) * gt, h))
        last = jnp.where(causal, s[:, t * tile :], MASKED)
        return [s[:, : t * tile], last] if t else [last]

    def finish(h, t, held):
        values = [part(v_ref, 0, t * gt, h)] if t else []
        values.append(part(v_ref, t * gt, gt, h))
        out = softmax_sum(held, values, scale2)
        out_ref[t * gt : (t + 1) * gt, :, h * dh : (h + 1) * dh] = out.reshape(gt, per, dh)

    run_tiles(width // dh, shards // gt, get_scores, finish)


def half_kernel(tile, scale2, dh, core_ref, q_ref, k_ref, v_ref, k2_ref, v2_ref, prev_ref, out_ref):
    shards, piece, width = q_ref.shape
    gt = tile // piece
    core = core_ref[0]
    key = lax.broadcasted_iota(jnp.int32, (tile, tile), 1)
    query = lax.broadcasted_iota(jnp.int32, (tile, tile), 0)
    causal = key <= query
    causal2 = key // piece < query // piece + core
    part = lambda ref, lo, n, h: ref[lo : lo + n, :, h * dh : (h + 1) * dh].reshape(n * piece, dh)

    def get_scores(h, t):
        q = part(q_ref, t * gt, gt, h)
        out = []
        for ref, mask in ((k_ref, causal), (k2_ref, causal2)):
            s = scores(q, part(ref, 0, (t + 1) * gt, h))
            out += [s[:, : t * tile]] if t else []
            out.append(jnp.where(mask, s[:, t * tile :], MASKED))
        return out

    def finish(h, t, held):
        values = []
        for ref in (v_ref, v2_ref):
            values += [part(ref, 0, t * gt, h)] if t else []
            values.append(part(ref, t * gt, gt, h))
        out = softmax_sum(held, values, scale2)
        out_ref[t * gt : (t + 1) * gt, :, h * dh : (h + 1) * dh] = out.reshape(gt, piece, dh)

    run_tiles(width // dh, shards // gt, get_scores, finish)


def attention(qkv, kv_own, kv_other, core, heads, dh):
    shards, per_shard = qkv.shape[:2]
    piece = kv_own.shape[1]
    n_whole, n_half = shards * 2 * piece, shards * piece
    tile = 256
    scale2 = float(dh**-0.5 * 1.4426950408889634)
    group = 2
    width = group * dh
    steps = heads // group
    params = pltpu.CompilerParams(vmem_limit_bytes=VMEM_LIMIT)
    out_shape = jax.ShapeDtypeStruct((shards, per_shard, heads * dh), jnp.bfloat16)
    whole = lambda third: pl.BlockSpec((shards, 2 * piece, width), lambda h: (0, 0, third * steps + h))
    out = pl.pallas_call(
        functools.partial(whole_kernel, tile, scale2, dh),
        grid=(steps,),
        in_specs=[whole(0), whole(1), whole(2)],
        out_specs=whole(0),
        out_shape=out_shape,
        compiler_params=params,
        cost_estimate=pl.CostEstimate(
            flops=8 * n_whole * n_whole * heads * dh, bytes_accessed=8 * n_whole * heads * dh, transcendentals=0
        ),
        name="attend_whole",
    )(qkv, qkv, qkv)
    width, steps = 2 * width, steps // 2
    shared = pl.BlockSpec((shards, piece, width), lambda h: (0, 2, h))
    side = lambda second: pl.BlockSpec((shards, piece, width), lambda h: (0, 0, second * steps + h))
    return pl.pallas_call(
        functools.partial(half_kernel, tile, scale2, dh),
        grid=(steps,),
        in_specs=[
            pl.BlockSpec(memory_space=pltpu.SMEM),
            shared,
            side(0),
            side(1),
            side(0),
            side(1),
            pl.BlockSpec(memory_space=pl.ANY),
        ],
        out_specs=shared,
        out_shape=out_shape,
        input_output_aliases={6: 0},
        compiler_params=params,
        cost_estimate=pl.CostEstimate(
            flops=8 * n_half * n_half * heads * dh, bytes_accessed=12 * n_half * heads * dh, transcendentals=0
        ),
        name="attend_half",
    )(core, qkv, kv_own, kv_own, kv_other, kv_other, out)


def tail_kernel(nk, group, o_ref, x_ref, wo_ref, gm_ref, up_ref, down_ref, *refs):
    if len(refs) == 4:
        ga_ref, y_ref, r_ref, acc = refs
    else:
        ga_ref, (y_ref, r_ref, acc) = None, refs
    step = pl.program_id(1)
    groups, per, width = x_ref.shape
    sub = group * per
    starts = range(0, groups, group)
    rows = lambda lo: slice(lo * per, lo * per + sub)
    project = lambda lo, n: jnp.dot(flat(o_ref, lo, n), wo_ref[...], preferred_element_type=jnp.float32)
    up = lambda lo: jnp.dot(flat(r_ref, lo, group), up_ref[...], preferred_element_type=jnp.float32)

    def pipelined(issue, finish):
        held = issue(0)
        for lo in starts:
            ahead = issue(lo + group) if lo + group < groups else None
            finish(lo, held)
            held = ahead

    @pl.when(step == 0)
    def _():
        acc[...] = project(0, groups)

    @pl.when((step > 0) & (step < nk - 1))
    def _():
        acc[...] += project(0, groups)

    @pl.when(step == nk - 1)
    def _():
        def finish(lo, prod):
            total = acc[rows(lo), :] + prod
            h = (flat(x_ref, lo, group).astype(jnp.float32) + total).astype(jnp.bfloat16)
            y_ref[lo : lo + group] = h.reshape(group, per, width)
            r_ref[lo : lo + group] = norm_rows(h.astype(jnp.float32), gm_ref[...]).reshape(group, per, width)

        pipelined(lambda lo: project(lo, group), finish)

    def add_block(first):
        def finish(lo, u):
            z = jax.nn.gelu(u, approximate=True).astype(jnp.bfloat16)
            prod = jnp.dot(z, down_ref[...], preferred_element_type=jnp.float32)
            if first:
                acc[rows(lo), :] = prod
            else:
                acc[rows(lo), :] += prod

        pipelined(up, finish)

    pl.when(step == nk)(lambda: add_block(True))
    pl.when(step > nk)(lambda: add_block(False))

    @pl.when(step == pl.num_programs(1) - 1)
    def _():
        for lo in range(groups):
            y = (y_ref[lo].astype(jnp.float32) + acc[lo * per : (lo + 1) * per, :]).astype(jnp.bfloat16)
            y_ref[lo] = y
            if ga_ref is not None:
                r_ref[lo] = norm_rows(y.astype(jnp.float32), ga_ref[...])


def layer_tail(o, x, w_out, gain_mlp, w_up, w_down, gain_next, layer, part=None):
    shards, per_shard, width = x.shape
    depth = o.shape[2]
    ff = w_up.shape[2]
    tf = tk = 1024
    nk = depth // tk
    early = lambda s: jnp.minimum(s, nk - 1)
    late = lambda s: jnp.maximum(s - nk, 0)
    gain_spec = pl.BlockSpec((1, width), lambda m, s: (0, 0))
    if part is None:
        blocks, block, group = 2, (shards // 2, per_shard), shards // 4
        place = lambda m: (m, 0)
        out_row = pl.BlockSpec((*block, width), lambda m, s: (m, 0, 0))
        extra, extra_specs = [gain_next], [gain_spec]
        out_shape = [jax.ShapeDtypeStruct(x.shape, jnp.bfloat16)] * 2
        scratch = []
    else:
        blocks, per, run = part
        block, group = (shards // blocks, per), shards // (2 * blocks)
        place = lambda m: (m, run)
        out_row = pl.BlockSpec((*block, width), lambda m, s: (m, 0, 0))
        extra, extra_specs = [], []
        out_shape = [jax.ShapeDtypeStruct((shards, per, width), jnp.bfloat16)]
        scratch = [pltpu.VMEM((*block, width), jnp.bfloat16)]
    rows = blocks * block[0] * block[1]
    return pl.pallas_call(
        functools.partial(tail_kernel, nk, group),
        grid=(blocks, nk + ff // tf),
        in_specs=[
            pl.BlockSpec((*block, tk), lambda m, s: (*place(m), early(s))),
            pl.BlockSpec((*block, width), lambda m, s: (*place(m), 0)),
            pl.BlockSpec((None, tk, width), lambda m, s: (layer, early(s), 0)),
            gain_spec,
            pl.BlockSpec((None, width, tf), lambda m, s: (layer, 0, late(s))),
            pl.BlockSpec((None, tf, width), lambda m, s: (layer, late(s), 0)),
            *extra_specs,
        ],
        out_specs=[out_row] * len(out_shape),
        out_shape=out_shape,
        scratch_shapes=[*scratch, pltpu.VMEM((block[0] * block[1], width), jnp.float32)],
        compiler_params=pltpu.CompilerParams(vmem_limit_bytes=VMEM_LIMIT),
        cost_estimate=pl.CostEstimate(
            flops=rows * width * (4 * ff + 2 * depth), bytes_accessed=width * (4 * ff + 2 * depth), transcendentals=0
        ),
        name="layer_tail",
    )(o, x, w_out, gain_mlp, w_up, w_down, *extra)


def solution(mesh):
    n_seq = mesh.shape["seq"]
    n_pair = n_seq // 2
    tok_spec = P(None, ("data", "seq"), None)
    in_specs = (tok_spec, P(("data", "seq"))) + (P(),) * 8
    partner = [(i, i ^ 1) for i in range(n_seq)]

    def device_fn(x_loc, pos_loc, w_query, w_key, w_value, w_out, w_up, w_down, g_attn, g_mlp):
        n_layers, _, heads, dh = w_query.shape
        n_batch, shard, width = x_loc.shape
        per = n_batch // n_pair
        assert per * n_pair == n_batch and per == 3
        piece = shard // 2
        core = lax.rem(lax.axis_index("seq"), 2)
        exchange = lambda a: lax.all_to_all(a, "seq", 0, 0, tiled=True)

        pos = exchange(jnp.broadcast_to(pos_loc, (n_seq, shard)))
        by_chip = x_loc.reshape(n_pair, per, shard, width)
        pos, send = lax.optimization_barrier((pos, by_chip[:, 2].reshape(n_seq, piece, width)))
        shared_x = exchange(send)
        shared_x, send = lax.optimization_barrier((shared_x, by_chip[:, :2].reshape(n_seq, shard, width)))
        whole_x = exchange(send)

        pos_shared = lax.dynamic_index_in_dim(pos.reshape(n_seq, 2, piece), core, axis=1, keepdims=False)
        inv_freq = ROPE_BASE ** (-jnp.arange(dh // 2, dtype=jnp.float32) * (2.0 / dh))
        angles = jnp.concatenate([pos, pos_shared], axis=1).astype(jnp.float32)[..., None] * inv_freq
        cos, sin = jnp.cos(angles), jnp.sin(angles)
        cos = jnp.concatenate([cos, cos], axis=-1)
        sin = jnp.concatenate([-sin, sin], axis=-1)
        core_arr = core.astype(jnp.int32).reshape(1)
        w_out2 = w_out.reshape(n_layers, heads * dh, width)

        first_args = (w_query, w_key, w_value, cos, sin, g_attn[0][None])
        qkv, hidden, kv_own = qkv_first(shared_x, 2, [], *first_args, True)
        qkv, hidden = qkv_first(whole_x, 0, [qkv, hidden], *first_args, False)
        for layer in range(n_layers):
            if layer:
                qkv, kv_own = qkv_later(normed, w_query, w_key, w_value, cos, sin, layer, piece)
            kv_other = lax.ppermute(kv_own, "seq", partner)
            attn = attention(qkv, kv_own, kv_other, core_arr, heads, dh)
            tail_args = (attn, hidden, w_out2, g_mlp[layer][None], w_up, w_down)
            if layer < n_layers - 1:
                hidden, normed = layer_tail(*tail_args, g_attn[layer + 1][None], layer)

        (y_whole,) = layer_tail(*tail_args, None, n_layers - 1, (2, shard, 0))
        y_whole = exchange(y_whole)
        (y_shared,) = layer_tail(*tail_args, None, n_layers - 1, (1, piece, 2))
        y_whole, y_shared = lax.optimization_barrier((y_whole, y_shared))
        y_shared = exchange(y_shared)
        whole = y_whole.reshape(n_pair, 2, shard, width)
        shared = y_shared.reshape(n_pair, 1, shard, width)
        return jnp.concatenate([whole, shared], axis=1).reshape(n_batch, shard, width)

    return jax.shard_map(device_fn, mesh=mesh, in_specs=in_specs, out_specs=tok_spec, check_vma=False)
```
